32 devices in a mesh: depth: 2 (over y), row: 4 (over z), col: 4 (over x, core).
Axes of the slice: x: 2, y: 2, z: 4, core: 2. Of those that a mesh axis runs over, the one named last changes fastest.
Arguments:
- features: bfloat16 [16, 576, 1152], P('row', 'col', 'depth'), may hold values from -6 to 6
- w_in: bfloat16 [1152, 4096], P('depth'), may hold values from -0.1875 to 0.1875
- b_in: float32 [4096], replicated, may hold values from -4 to 4
- w_out: bfloat16 [4096, 4096], P('row', 'depth'), may hold values from -0.09375 to 0.09375
- b_out: float32 [4096], P('depth'), may hold values from -3 to 3
- text: bfloat16 [16, 448, 4096], P(('row', 'col'), None, 'depth'), may hold values from -6 to 6
- offsets: int32 [16], P(('row', 'col')), may hold values from 0 to 448
Outputs:
- sequences: bfloat16 [16, 1024, 4096], P(('row', 'col'), None, 'depth')
The draws below stay inside these ranges and needn't reach their ends.
Inputs may be any that keep to these rules, and one draw needn't show every extreme that they name: offsets[i] is where image i's first patch stands in sequence i.
All inputs are finite; a program needn't handle non-finite values.
Results may differ from the reference program's by a relative error of at most 0.007.
Values may be sent and summed in bfloat16 or wider, within the bound.
No kernel may reach another device: no remote copies, remote signals or barrier semaphores. Data moves between devices by JAX's collectives and lax.ppermute only.
A program may use at most 128 MiB of HBM per device.

```python
import jax
import jax.numpy as jnp
from jax import lax

C = 1152
H = 4096
D = 4096
PATCHES = 576
TEXT = 448
IMAGES = 16


def set_ends(entries, own_key, least, largest):
    longest = entries.shape.index(max(entries.shape))
    spots = []
    for shift in (0, 1):
        where = [jax.random.randint(jax.random.fold_in(own_key, axis), (), 0, length) for axis, length in enumerate(entries.shape)]
        where[longest] = (where[longest] + shift) % entries.shape[longest]
        spots.append(tuple(where))
    return entries.at[spots[0]].set(least).at[spots[1]].set(largest)


def shard_levels(stream_key, extent, pieces, smallest, high):
    def one(position, blocks):
        heights = jax.random.uniform(jax.random.fold_in(jax.random.fold_in(stream_key, 6), position), (blocks,), jnp.float32, smallest / len(pieces), high / len(pieces))
        return jnp.repeat(jnp.exp(heights), extent[position] // blocks).reshape((-1,) + (1,) * (len(extent) - position - 1))

    gain = one(*pieces[0])
    for cut in pieces[1:]:
        gain = gain * one(*cut)
    return gain


def scatter_about(key, dims, scale, reach, pieces=(), held_as=jnp.bfloat16):
    drawn = scale * jax.random.normal(key, dims, jnp.float32)
    if pieces:
        drawn = drawn * shard_levels(key, dims, pieces, -0.22, 0.18)
    return jnp.clip(drawn, -reach, reach).astype(held_as)


def setup_inputs(seed: int = 0) -> dict:
    streams_of = jax.random.split(jax.random.key(seed), 8)
    return {
        "features": scatter_about(streams_of[0], (IMAGES, PATCHES, C), 1.0, 6.0, ((0, 4), (1, 4), (2, 2))),
        "w_in": scatter_about(streams_of[1], (C, H), C ** -0.5, 0.1875, ((0, 2),)),
        "b_in": scatter_about(streams_of[2], (H,), 1.0, 4.0, (), jnp.float32),
        "w_out": scatter_about(streams_of[3], (H, D), H ** -0.5, 0.09375, ((0, 4), (1, 2))),
        "b_out": scatter_about(streams_of[4], (D,), 0.5, 3.0, ((0, 2),), jnp.float32),
        "text": scatter_about(streams_of[5], (IMAGES, TEXT, D), 1.0, 6.0, ((0, 16), (2, 2))),
        "offsets": set_ends(jax.random.randint(streams_of[6], (IMAGES,), 0, TEXT + 1), jax.random.fold_in(streams_of[6], 1), 0, TEXT).astype(jnp.int32),
    }


def place_image(image_rows, text_rows, offset):
    patch_count = image_rows.shape[0]
    text_count = text_rows.shape[0]
    width = image_rows.shape[1]
    length = patch_count + text_count
    positions = jnp.arange(length, dtype=jnp.int32)
    zeros_text = jnp.zeros((text_count, width), image_rows.dtype)
    padded = jnp.concatenate([zeros_text, image_rows, zeros_text], 0)
    shifted = lax.dynamic_slice_in_dim(padded, (text_count - offset).astype(jnp.int32), length, 0)
    zeros_patch = jnp.zeros((patch_count, width), text_rows.dtype)
    early = jnp.concatenate([text_rows, zeros_patch], 0)
    later = jnp.concatenate([zeros_patch, text_rows], 0)
    inside = (positions >= offset) & (positions < offset + patch_count)
    before = positions < offset
    return jnp.where(inside[:, None], shifted, jnp.where(before[:, None], early, later))


def reference(features, w_in, b_in, w_out, b_out, text, offsets):
    half_width = C // 2

    def one_image(packed):
        image, text_rows, offset = packed
        first = jnp.dot(image[:, :half_width], w_in[:half_width], preferred_element_type=jnp.float32).astype(jnp.bfloat16)
        second = jnp.dot(image[:, half_width:], w_in[half_width:], preferred_element_type=jnp.float32).astype(jnp.bfloat16)
        first, second = lax.optimization_barrier((first, second))
        pre = first.astype(jnp.float32) + second.astype(jnp.float32) + b_in
        hidden = jax.nn.gelu(pre, approximate=False).astype(jnp.bfloat16)
        projected = (jnp.dot(hidden, w_out, preferred_element_type=jnp.float32) + b_out).astype(jnp.bfloat16)
        return place_image(projected, text_rows, offset)

    return lax.map(one_image, (features, text, offsets))
```

```python
import functools
import math

import jax
import jax.numpy as jnp
from jax import lax
from jax.experimental import pallas as pl
from jax.experimental.pallas import tpu as pltpu
from jax.sharding import PartitionSpec as P


CORES = 2
PIECES = 2
SQRT_HALF = math.sqrt(0.5)
CORE, OFFSET, PIECE = 0, 1, 2
F32, BF16 = jnp.float32, jnp.bfloat16


def tile_of(extent, largest, unit):
    size = largest // unit * unit
    while extent % size:
        size -= unit
    return size


def hidden_kernel(scalars, *refs):
    count = (len(refs) - 2) // 2
    tokens, weights, bias, out = refs[:count], refs[count : 2 * count], refs[-2], refs[-1]
    width = out.shape[1]
    step = min(width, 256)
    for start in range(0, width, step):
        columns = slice(start, start + step)
        pre = bias[0, :, columns]
        for value, weight in zip(tokens, weights):
            pre = pre + jnp.dot(value[...], weight[:, columns], preferred_element_type=F32)
        out[:, columns] = (0.5 * pre * (1.0 + lax.erf(pre * SQRT_HALF))).astype(out.dtype)


def hidden_part(scalars, tokens, weights, bias, slot):
    count, inner = tokens[0].shape
    width = weights[0].shape[1]
    tile = tile_of(count, 576, 16)
    flops = 2 * count * inner * width * len(tokens)
    return pl.pallas_call(
        hidden_kernel,
        grid_spec=pltpu.PrefetchScalarGridSpec(
            num_scalar_prefetch=1,
            grid=(count // tile,),
            in_specs=[pl.BlockSpec((tile, inner), lambda i, s: (i, 0))] * len(tokens)
            + [pl.BlockSpec((inner, width), lambda i, s: (0, 0))] * len(weights)
            + [pl.BlockSpec((1, 1, width), lambda i, s: (s[slot], 0, 0))],
            out_specs=pl.BlockSpec((tile, width), lambda i, s: (i, 0)),
        ),
        out_shape=jax.ShapeDtypeStruct((count, width), BF16),
        cost_estimate=pl.CostEstimate(flops=flops, bytes_accessed=4 * count * inner, transcendentals=0),
        compiler_params=pltpu.CompilerParams(vmem_limit_bytes=8 * 2**20),
    )(scalars, *tokens, *weights, bias)


def product_kernel(layout, tile, carry, scalars, *refs):
    refs = list(refs)
    if carry:
        refs.pop(0)
    stages = []
    for entry in layout:
        own, other = refs.pop(0), refs.pop(0)
        stages.append((own, other, [refs.pop(0) for _ in entry or (0,)]))
    out = refs.pop(0)
    held = [refs.pop(0) for _ in layout]
    sems = refs.pop(0)
    core = scalars[CORE]

    @pl.when(pl.program_id(0) == 0)
    def _():
        copies = []
        for entry, (_, _, parts), buffer in zip(layout, stages, held):
            width = buffer.shape[1]
            for number, part in enumerate(parts):
                if entry is None:
                    part = part.at[:, pl.ds(pl.multiple_of(core * width, width), width)]
                    target = buffer
                else:
                    slot, start = entry[number]
                    height = part.shape[0]
                    target = buffer.at[pl.ds(pl.multiple_of(scalars[slot] + start, height), height)]
                copy = pltpu.make_async_copy(part, target, sems.at[len(copies)])
                copy.start()
                copies.append(copy)
        for copy in copies:
            copy.wait()

    window = pl.ds(pl.multiple_of(pl.program_id(0) * tile, tile), tile)
    total = out[window, :] if carry else None
    for entry, (own, other, parts), buffer in zip(layout, stages, held):
        half = own.shape[1]
        for value, side in ((own, core), (other, 1 - core)):
            first = pl.multiple_of(side * half, half)
            term = jnp.dot(value[...], buffer[pl.ds(first, half), :], preferred_element_type=F32)
            total = term if total is None else total + term
    out[window, :] = total


def pieces_sum(entry, scalars, own, other, parts):
    half = own.shape[1]
    total = None
    for (slot, start), part in zip(entry, parts):
        height = part.shape[0]
        mine = scalars[slot] // half == scalars[CORE]
        columns = slice(start % half, start % half + height)
        value = jnp.where(mine, own[:, columns], other[:, columns])
        term = jnp.dot(value, part[...], preferred_element_type=F32)
        total = term if total is None else total + term
    return total


def third_kernel(entry, tile, scalars, carried, own, other, *refs):
    parts, out = refs[:-1], refs[-1]
    window = pl.ds(pl.multiple_of(pl.program_id(0) * tile, tile), tile)
    out[window, :] = out[window, :] + pieces_sum(entry, scalars, own, other, parts)


def finish_kernel(entry, image, scalars, carried, bias, own, other, *refs):
    parts, out = refs[:-1], refs[-1]
    side = scalars[CORE] if image else 1 - scalars[CORE]
    tile = out.shape[0]
    steps = pl.num_programs(0)
    first = pl.multiple_of((side * steps + pl.program_id(0)) * tile, tile)
    total = carried[pl.ds(first, tile), :] + bias[...] + pieces_sum(entry, scalars, own, other, parts)
    out[...] = total.astype(out.dtype)


def product(scalars, stages, carried):
    count, half = stages[0][0].shape
    block = half * CORES
    tile = tile_of(count, 576, 16)
    operands, in_specs, scratch, layout = [], [], [], []
    for own, other, whole, pieces in stages:
        width = pieces[0][0].shape[1] if pieces else whole.shape[1] // CORES
    if carried is not None:
        operands.append(carried)
        in_specs.append(pl.BlockSpec(memory_space=pltpu.VMEM))
    copies = 0
    for own, other, whole, pieces in stages:
        operands += [own, other]
        in_specs += [pl.BlockSpec((tile, half), lambda i, s: (i, 0))] * 2
        if whole is not None:
            operands.append(whole)
            layout.append(None)
        else:
            operands += [p[0] for p in pieces]
            layout.append(tuple((p[1], p[2]) for p in pieces))
        count_here = max(1, len(pieces))
        in_specs += [pl.BlockSpec(memory_space=pl.ANY)] * count_here
        copies += count_here
        scratch.append(pltpu.VMEM((block, width), BF16))
    scratch.append(pltpu.SemaphoreType.DMA((copies,)))
    flops = 2 * count * block * width * len(stages)
    return pl.pallas_call(
        functools.partial(product_kernel, tuple(layout), tile, carried is not None),
        grid_spec=pltpu.PrefetchScalarGridSpec(
            num_scalar_prefetch=1,
            grid=(count // tile,),
            in_specs=in_specs,
            out_specs=pl.BlockSpec(memory_space=pltpu.VMEM),
            scratch_shapes=scratch,
        ),
        out_shape=jax.ShapeDtypeStruct((count, width), F32),
        input_output_aliases={} if carried is None else {1: 0},
        cost_estimate=pl.CostEstimate(flops=flops, bytes_accessed=8 * count * width, transcendentals=0),
        compiler_params=pltpu.CompilerParams(vmem_limit_bytes=8 * 2**20),
    )(scalars, *operands)


def third(scalars, carried, own, other, pieces):
    count, half = own.shape
    width = carried.shape[1]
    tile = tile_of(count, 576, 16)
    height = pieces[0][0].shape[0]
    return pl.pallas_call(
        functools.partial(third_kernel, tuple((p[1], p[2]) for p in pieces), tile),
        grid_spec=pltpu.PrefetchScalarGridSpec(
            num_scalar_prefetch=1,
            grid=(count // tile,),
            in_specs=[pl.BlockSpec(memory_space=pltpu.VMEM)]
            + [pl.BlockSpec((tile, half), lambda i, s: (i, 0))] * 2
            + [pl.BlockSpec((height, width), lambda i, s: (0, 0))] * len(pieces),
            out_specs=pl.BlockSpec(memory_space=pltpu.VMEM),
        ),
        out_shape=jax.ShapeDtypeStruct((count, width), F32),
        input_output_aliases={1: 0},
        cost_estimate=pl.CostEstimate(
            flops=2 * count * height * width * len(pieces), bytes_accessed=8 * count * width, transcendentals=0
        ),
        compiler_params=pltpu.CompilerParams(vmem_limit_bytes=8 * 2**20),
    )(scalars, carried, own, other, *[p[0] for p in pieces])


def finish(scalars, image, carried, bias, own, other, pieces):
    count, half = own.shape
    width = carried.shape[1]
    rows = count // CORES
    tile = tile_of(rows, 576, 16)
    steps = rows // tile

    def spot(i, s):
        return ((s[CORE] if image else 1 - s[CORE]) * steps + i, 0)

    height = pieces[0][0].shape[0]
    return pl.pallas_call(
        functools.partial(finish_kernel, tuple((p[1], p[2]) for p in pieces), image),
        grid_spec=pltpu.PrefetchScalarGridSpec(
            num_scalar_prefetch=1,
            grid=(steps,),
            in_specs=[
                pl.BlockSpec(memory_space=pltpu.VMEM),
                pl.BlockSpec((1, width), lambda i, s: (0, 0)),
                pl.BlockSpec((tile, half), spot),
                pl.BlockSpec((tile, half), spot),
            ]
            + [pl.BlockSpec((height, width), lambda i, s: (0, 0))] * len(pieces),
            out_specs=pl.BlockSpec((tile, width), lambda i, s: (i, 0)),
        ),
        out_shape=jax.ShapeDtypeStruct((rows, width), BF16),
        cost_estimate=pl.CostEstimate(
            flops=2 * rows * height * width * len(pieces), bytes_accessed=6 * rows * width, transcendentals=0
        ),
        compiler_params=pltpu.CompilerParams(vmem_limit_bytes=8 * 2**20),
    )(scalars, carried, bias, own, other, *[p[0] for p in pieces])


def place_kernel(scalars, text, image, *refs):
    out, held, padded = refs[-3:]
    text_count, patch_count, width = text.shape[1], image.shape[0], image.shape[1]
    offset = scalars[OFFSET]
    shift = lax.rem(offset, 8)
    first = offset - shift
    chunk = tile_of(patch_count, 64, 8)
    sublane = lax.broadcasted_iota(jnp.int32, (1, 8, 128), 1)
    for start in range(0, width, 128):
        lanes = slice(start, start + 128)
        words = text[0, :, lanes].astype(F32)
        held[0:text_count, lanes] = words
        held[patch_count : patch_count + text_count, lanes] = words
        padded[8 : 8 + patch_count, lanes] = image[:, lanes].astype(F32)
        for row in range(0, patch_count + 8, chunk):
            size = min(chunk, patch_count + 8 - row)
            values = padded[row : row + size + 8, lanes].reshape(-1, 8, 128)
            turned = pltpu.roll(values, shift, 1)
            moved = jnp.where(sublane < shift, turned[:-1], turned[1:])
            window = pl.ds(pl.multiple_of(first + row, 8), size)
            if row == 0 or row + size > patch_count:
                place = lax.broadcasted_iota(jnp.int32, moved.shape, 0) * 8 + sublane + row
                kept = held[window, lanes].reshape(-1, 8, 128)
                moved = jnp.where((place >= shift) & (place < shift + patch_count), moved, kept)
            held[window, lanes] = moved.reshape(size, 128)
    out[0] = held[0 : text_count + patch_count].astype(out.dtype)


def place(scalars, text, image, sequence, mine):
    patch_count, half = image.shape
    text_count, width = text.shape[1], text.shape[2]
    length = text_count + patch_count
    tile = tile_of(half, 256, 128)
    steps = half // tile

    def side(i, s):
        return (s[CORE] if mine else 1 - s[CORE]) * steps + i

    operands = [text, image] + ([] if sequence is None else [sequence])
    return pl.pallas_call(
        place_kernel,
        grid_spec=pltpu.PrefetchScalarGridSpec(
            num_scalar_prefetch=1,
            grid=(steps,),
            in_specs=[
                pl.BlockSpec((1, text_count, tile), lambda i, s: (0, 0, side(i, s))),
                pl.BlockSpec((patch_count, tile), lambda i, s: (0, i)),
            ]
            + ([] if sequence is None else [pl.BlockSpec(memory_space=pl.ANY)]),
            out_specs=pl.BlockSpec((1, length, tile), lambda i, s: (0, 0, side(i, s))),
            scratch_shapes=[pltpu.VMEM((length + 8, tile), F32), pltpu.VMEM((patch_count + 16, tile), F32)],
        ),
        out_shape=jax.ShapeDtypeStruct((1, length, width), BF16),
        input_output_aliases={} if sequence is None else {3: 0},
        cost_estimate=pl.CostEstimate(flops=10**9, bytes_accessed=4 * length * half, transcendentals=0),
        compiler_params=pltpu.CompilerParams(vmem_limit_bytes=8 * 2**20),
    )(scalars, *operands)


def edge_pairs(rows, distance, parity):
    pairs = []
    for i in range(parity, rows - 1, 2):
        if i >= distance - 1:
            pairs.append((i, i + 1))
        if i + 1 <= rows - distance:
            pairs.append((i + 1, i))
    return pairs


def full_pairs(rows, cols, distance, parity):
    busy = {min(pair) for pair in edge_pairs(rows, distance, parity)}
    pairs = []
    for row in range(rows):
        other = row + 1 if row in busy else row - 1 if row - 1 in busy else None
        for col in range(cols):
            target = row * cols + (col ^ 1) if other is None else other * cols + col
            pairs.append((row * cols + col, target))
    return pairs if busy else []


def arrivals(rows, row):
    order = []
    for distance in range(1, rows):
        for parity in (0, 1):
            for source, target in edge_pairs(rows, distance, parity):
                if target == row:
                    order.append((parity, distance, row - distance if source < target else row + distance))
    return order


def at_row(row, values):
    result = values[-1]
    for index in range(len(values) - 2, -1, -1):
        result = jnp.where(row == index, values[index], result)
    return result


def choose_kernel(which, *refs):
    choices, out, sem = refs[:-2], refs[-2], refs[-1]
    for index, choice in enumerate(choices):

        @pl.when(which[0] == index)
        def _():
            pltpu.make_async_copy(choice, out, sem).start()

    pltpu.make_async_copy(choices[0], out, sem).wait()


def by_row(row, choices):
    distinct = []
    for choice in choices:
        if not any(choice is d for d in distinct):
            distinct.append(choice)
    if len(distinct) == 1:
        return distinct[0]
    which = at_row(row, [next(i for i, d in enumerate(distinct) if d is choice) for choice in choices])
    shape = distinct[0].shape
    return pl.pallas_call(
        choose_kernel,
        grid_spec=pltpu.PrefetchScalarGridSpec(
            num_scalar_prefetch=1,
            grid=(),
            in_specs=[pl.BlockSpec(memory_space=pl.ANY)] * len(distinct),
            out_specs=pl.BlockSpec(shape, lambda s: (0, 0)),
            scratch_shapes=[pltpu.SemaphoreType.DMA],
        ),
        out_shape=jax.ShapeDtypeStruct(shape, distinct[0].dtype),
        cost_estimate=pl.CostEstimate(flops=10**9, bytes_accessed=8 * shape[0] * shape[1], transcendentals=0),
        compiler_params=pltpu.CompilerParams(vmem_limit_bytes=8 * 2**20),
    )(which.astype(jnp.int32).reshape(1), *distinct)


def on_device(features, w_in, b_in, w_out, b_out, text, offsets):
    depths, rows, cols = lax.axis_size("depth"), lax.axis_size("row"), lax.axis_size("col")
    chips = cols // CORES
    row, col = lax.axis_index("row"), lax.axis_index("col")
    chip, core = col // CORES, col % CORES
    _, patch_count, part_width = features.shape
    block, out_width = w_out.shape
    half_block, half_out = block // CORES, out_width // CORES
    piece_rows = block // chips
    height = piece_rows // PIECES

    def to_core(value):
        return lax.ppermute(value, "col", [(i, i ^ 1) for i in range(cols)])

    def to_chip(value, step):
        return lax.ppermute(value, "col", [(i, (i + step * CORES) % cols) for i in range(cols)])

    def to_depth(value, step):
        return lax.ppermute(value, "depth", [(i, (i + step) % depths) for i in range(depths)])

    tables = [arrivals(rows, i) for i in range(rows)]
    blocks = [row] + [at_row(row, [t[k][2] for t in tables]) for k in range(rows - 1)]

    pieces = [
        lax.dynamic_slice(w_out, (chip * piece_rows + j * height, core * half_out), (height, half_out))
        for j in range(PIECES)
    ]
    moved = {(parity, 0, j): pieces[j] for parity in (0, 1) for j in range(PIECES)}
    for distance in range(1, rows):
        for j in range(PIECES):
            for parity in (0, 1):
                pairs = full_pairs(rows, cols, distance, parity)
                if pairs:
                    held = moved[1 - parity, distance - 1, j]
                    moved[parity, distance, j] = lax.ppermute(held, ("row", "col"), pairs)
    stage_pieces = [None]
    starts = [chip * piece_rows] + [(chip - step) % chips * piece_rows for step in range(1, chips)]
    scalars = jnp.stack([core, offsets[0], *starts, *[b * CORES + core for b in blocks]])
    scalars = scalars.astype(jnp.int32)
    for k in range(1, rows):
        own, received = [], []
        for j in range(PIECES):
            chosen = by_row(row, [moved[t[k - 1][:2] + (j,)] for t in tables])
            own.append((chosen, PIECE, j * height))
            for step in range(1, chips):
                received.append((to_chip(chosen, step), PIECE + step, j * height))
        stage_pieces.append(own + received)

    by_chip = features.reshape(chips, CORES, patch_count, part_width)
    sent = [
        lax.dynamic_index_in_dim(by_chip, (chip + step) % chips, 0, keepdims=False) for step in range(chips)
    ]
    tokens = []
    for away in range(depths):
        got = []
        for step in range(chips):
            pairs = [
                (d * cols + i, (d + away) % depths * cols + (i + step * CORES) % cols)
                for d in range(depths)
                for i in range(cols)
            ]
            got.append(lax.ppermute(sent[step], ("depth", "col"), pairs) if away or step else sent[0])
        with_other = []
        for step in range(chips):
            value = got[step][:, None]
            other = to_core(value)
            with_other.append((value, other))
        sides = [jnp.where(core == 0, jnp.stack(pair, 2), jnp.stack(pair[::-1], 2)) for pair in with_other]
        if chips == 2:
            part = jnp.where(chip == 0, jnp.concatenate(sides, 1), jnp.concatenate(sides[::-1], 1))
        else:
            part = jnp.zeros((CORES, chips, CORES, patch_count, part_width), features.dtype)
            for step in range(chips):
                part = lax.dynamic_update_slice(part, sides[step], (0, (chip - step) % chips, 0, 0, 0))
        tokens.append(part.reshape(-1, part_width))

    bias_in = b_in.reshape(rows * CORES, 1, half_block)
    hidden = []
    columns = [b * block + core * half_block for b in blocks]
    cuts = [lax.dynamic_slice_in_dim(w_in, columns[0], half_block, 1)]
    later = lax.optimization_barrier((w_in, cuts[0]))[0]
    cuts += [lax.dynamic_slice_in_dim(later, column, half_block, 1) for column in columns[1:]]
    for k in range(rows):
        own = cuts[k]
        weights = [own] + [to_depth(own, step) for step in range(1, depths)]
        value = hidden_part(scalars, tokens, weights, bias_in, PIECE + chips + k)
        hidden.append((value, to_core(value)))

    bias_out = lax.dynamic_slice_in_dim(b_out, core * half_out, half_out).reshape(1, half_out)
    split = chips == CORES and height % 128 == 0
    for k in range(rows - split):
        stage = (*hidden[k], w_out if k == 0 else None, stage_pieces[k] or [])
        total = product(scalars, [stage], total if k else None)
    if split:
        last = stage_pieces[-1]
        total = third(scalars, total, *hidden[-1], last[:-1])
        sent = finish(scalars, 0, total, bias_out, *hidden[-1], last[-1:])
        kept = finish(scalars, 1, total, bias_out, *hidden[-1], last[-1:])
    else:
        result = (total + bias_out).astype(BF16).reshape(CORES, -1, half_out)
        sent = lax.dynamic_index_in_dim(result, 1 - core, 0, keepdims=False)
        kept = lax.dynamic_index_in_dim(result, core, 0, keepdims=False)
    arrived = to_core(sent)
    sequence = place(scalars, text, kept, None, True)
    return place(scalars, text, arrived, sequence, False)


def solution(mesh):
    return jax.shard_map(
        on_device,
        mesh=mesh,
        in_specs=(
            P("row", "col", "depth"),
            P("depth", None),
            P(),
            P("row", "depth"),
            P("depth"),
            P(("row", "col"), None, "depth"),
            P(("row", "col")),
        ),
        out_specs=P(("row", "col"), None, "depth"),
        check_vma=False,
    )
```

```python
import functools
import math

import jax
import jax.numpy as jnp
from jax import lax
from jax.experimental import pallas as pl
from jax.experimental.pallas import tpu as pltpu
from jax.sharding import PartitionSpec as P


CORES = 2
PIECES = 2
SQRT_HALF = math.sqrt(0.5)
CORE, OFFSET, PIECE = 0, 1, 2
F32, BF16 = jnp.float32, jnp.bfloat16


def tile_of(extent, largest, unit):
    size = largest // unit * unit
    while extent % size:
        size -= unit
    return size


def hidden_kernel(scalars, *refs):
    count = (len(refs) - 2) // 2
    tokens, weights, bias, out = refs[:count], refs[count : 2 * count], refs[-2], refs[-1]
    inner, width = weights[0].shape
    step = min(width, 256)
    whole = inner // 256 * 256
    ends = None
    if whole < inner:
        ends = jnp.concatenate([value[:, whole:] for value in tokens], 1)
    for start in range(0, width, step):
        columns = slice(start, start + step)
        pre = bias[0, :, columns]
        for value, weight in zip(tokens, weights):
            pre = pre + jnp.dot(value[:, :whole], weight[:whole, columns], preferred_element_type=F32)
        if ends is not None:
            rest = jnp.concatenate([weight[whole:, columns] for weight in weights], 0)
            pre = pre + jnp.dot(ends, rest, preferred_element_type=F32)
        out[:, columns] = (0.5 * pre * (1.0 + lax.erf(pre * SQRT_HALF))).astype(out.dtype)


def hidden_part(scalars, tokens, weights, bias, slot):
    count, inner = tokens[0].shape
    width = weights[0].shape[1]
    tile = tile_of(count, 576, 16)
    flops = 2 * count * inner * width * len(tokens)
    return pl.pallas_call(
        hidden_kernel,
        grid_spec=pltpu.PrefetchScalarGridSpec(
            num_scalar_prefetch=1,
            grid=(count // tile,),
            in_specs=[pl.BlockSpec((tile, inner), lambda i, s: (i, 0))] * len(tokens)
            + [pl.BlockSpec((inner, width), lambda i, s: (0, 0))] * len(weights)
            + [pl.BlockSpec((1, 1, width), lambda i, s: (s[slot], 0, 0))],
            out_specs=pl.BlockSpec((tile, width), lambda i, s: (i, 0)),
        ),
        out_shape=jax.ShapeDtypeStruct((count, width), BF16),
        cost_estimate=pl.CostEstimate(flops=flops, bytes_accessed=4 * count * inner, transcendentals=0),
        compiler_params=pltpu.CompilerParams(vmem_limit_bytes=8 * 2**20),
    )(scalars, *tokens, *weights, bias)


def product_kernel(layout, tile, carry, scalars, *refs):
    refs = list(refs)
    if carry:
        refs.pop(0)
    stages = []
    for entry in layout:
        own, other = refs.pop(0), refs.pop(0)
        stages.append((own, other, [refs.pop(0) for _ in entry or (0,)]))
    out = refs.pop(0)
    held = [refs.pop(0) for _ in layout]
    sems = refs.pop(0)
    core = scalars[CORE]

    @pl.when(pl.program_id(0) == 0)
    def _():
        copies = []
        for entry, (_, _, parts), buffer in zip(layout, stages, held):
            width = buffer.shape[1]
            for number, part in enumerate(parts):
                if entry is None:
                    part = part.at[:, pl.ds(pl.multiple_of(core * width, width), width)]
                    target = buffer
                else:
                    slot, start = entry[number]
                    height = part.shape[0]
                    target = buffer.at[pl.ds(pl.multiple_of(scalars[slot] + start, height), height)]
                copy = pltpu.make_async_copy(part, target, sems.at[len(copies)])
                copy.start()
                copies.append(copy)
        for copy in copies:
            copy.wait()

    window = pl.ds(pl.multiple_of(pl.program_id(0) * tile, tile), tile)
    total = out[window, :] if carry else None
    for entry, (own, other, parts), buffer in zip(layout, stages, held):
        half = own.shape[1]
        for value, side in ((own, core), (other, 1 - core)):
            first = pl.multiple_of(side * half, half)
            term = jnp.dot(value[...], buffer[pl.ds(first, half), :], preferred_element_type=F32)
            total = term if total is None else total + term
    out[window, :] = total


def pieces_sum(entry, scalars, own, other, parts):
    half = own.shape[1]
    groups = []
    for (slot, start), part in zip(entry, parts):
        if groups and groups[-1][0] == slot and groups[-1][2] == start:
            groups[-1][2] += part.shape[0]
            groups[-1][3].append(part)
        else:
            groups.append([slot, start, start + part.shape[0], [part]])
    total = None
    for slot, start, stop, members in groups:
        mine = scalars[slot] // half == scalars[CORE]
        columns = slice(start % half, start % half + stop - start)
        value = jnp.where(mine, own[:, columns], other[:, columns])
        weights = [part[...] for part in members]
        weights = weights[0] if len(weights) == 1 else jnp.concatenate(weights, 0)
        term = jnp.dot(value, weights, preferred_element_type=F32)
        total = term if total is None else total + term
    return total


def third_kernel(entry, tile, scalars, carried, own, other, *refs):
    parts, out = refs[:-1], refs[-1]
    window = pl.ds(pl.multiple_of(pl.program_id(0) * tile, tile), tile)
    out[window, :] = out[window, :] + pieces_sum(entry, scalars, own, other, parts)


def finish_kernel(entry, image, scalars, carried, bias, own, other, *refs):
    parts, out = refs[:-1], refs[-1]
    side = scalars[CORE] if image else 1 - scalars[CORE]
    tile = out.shape[0]
    steps = pl.num_programs(0)
    first = pl.multiple_of((side * steps + pl.program_id(0)) * tile, tile)
    total = carried[pl.ds(first, tile), :] + bias[...] + pieces_sum(entry, scalars, own, other, parts)
    out[...] = total.astype(out.dtype)


def product(scalars, stages, carried):
    count, half = stages[0][0].shape
    block = half * CORES
    tile = tile_of(count, 576, 16)
    operands, in_specs, scratch, layout = [], [], [], []
    for own, other, whole, pieces in stages:
        width = pieces[0][0].shape[1] if pieces else whole.shape[1] // CORES
    if carried is not None:
        operands.append(carried)
        in_specs.append(pl.BlockSpec(memory_space=pltpu.VMEM))
    copies = 0
    for own, other, whole, pieces in stages:
        operands += [own, other]
        in_specs += [pl.BlockSpec((tile, half), lambda i, s: (i, 0))] * 2
        if whole is not None:
            operands.append(whole)
            layout.append(None)
        else:
            operands += [p[0] for p in pieces]
            layout.append(tuple((p[1], p[2]) for p in pieces))
        count_here = max(1, len(pieces))
        in_specs += [pl.BlockSpec(memory_space=pl.ANY)] * count_here
        copies += count_here
        scratch.append(pltpu.VMEM((block, width), BF16))
    scratch.append(pltpu.SemaphoreType.DMA((copies,)))
    flops = 2 * count * block * width * len(stages)
    return pl.pallas_call(
        functools.partial(product_kernel, tuple(layout), tile, carried is not None),
        grid_spec=pltpu.PrefetchScalarGridSpec(
            num_scalar_prefetch=1,
            grid=(count // tile,),
            in_specs=in_specs,
            out_specs=pl.BlockSpec(memory_space=pltpu.VMEM),
            scratch_shapes=scratch,
        ),
        out_shape=jax.ShapeDtypeStruct((count, width), F32),
        input_output_aliases={} if carried is None else {1: 0},
        cost_estimate=pl.CostEstimate(flops=flops, bytes_accessed=8 * count * width, transcendentals=0),
        compiler_params=pltpu.CompilerParams(vmem_limit_bytes=8 * 2**20),
    )(scalars, *operands)


def third(scalars, carried, own, other, pieces):
    count, half = own.shape
    width = carried.shape[1]
    tile = tile_of(count, 576, 16)
    height = sum(p[0].shape[0] for p in pieces)
    return pl.pallas_call(
        functools.partial(third_kernel, tuple((p[1], p[2]) for p in pieces), tile),
        grid_spec=pltpu.PrefetchScalarGridSpec(
            num_scalar_prefetch=1,
            grid=(count // tile,),
            in_specs=[pl.BlockSpec(memory_space=pltpu.VMEM)]
            + [pl.BlockSpec((tile, half), lambda i, s: (i, 0))] * 2
            + [pl.BlockSpec(p[0].shape, lambda i, s: (0, 0)) for p in pieces],
            out_specs=pl.BlockSpec(memory_space=pltpu.VMEM),
        ),
        out_shape=jax.ShapeDtypeStruct((count, width), F32),
        input_output_aliases={1: 0},
        cost_estimate=pl.CostEstimate(
            flops=2 * count * height * width, bytes_accessed=8 * count * width, transcendentals=0
        ),
        compiler_params=pltpu.CompilerParams(vmem_limit_bytes=8 * 2**20),
    )(scalars, carried, own, other, *[p[0] for p in pieces])


def finish(scalars, image, carried, bias, own, other, pieces):
    count, half = own.shape
    width = carried.shape[1]
    rows = count // CORES
    tile = tile_of(rows, 576, 16)
    steps = rows // tile

    def spot(i, s):
        return ((s[CORE] if image else 1 - s[CORE]) * steps + i, 0)

    height = sum(p[0].shape[0] for p in pieces)
    return pl.pallas_call(
        functools.partial(finish_kernel, tuple((p[1], p[2]) for p in pieces), image),
        grid_spec=pltpu.PrefetchScalarGridSpec(
            num_scalar_prefetch=1,
            grid=(steps,),
            in_specs=[
                pl.BlockSpec(memory_space=pltpu.VMEM),
                pl.BlockSpec((1, width), lambda i, s: (0, 0)),
                pl.BlockSpec((tile, half), spot),
                pl.BlockSpec((tile, half), spot),
            ]
            + [pl.BlockSpec(p[0].shape, lambda i, s: (0, 0)) for p in pieces],
            out_specs=pl.BlockSpec((tile, width), lambda i, s: (i, 0)),
        ),
        out_shape=jax.ShapeDtypeStruct((rows, width), BF16),
        cost_estimate=pl.CostEstimate(
            flops=2 * rows * height * width, bytes_accessed=6 * rows * width, transcendentals=0
        ),
        compiler_params=pltpu.CompilerParams(vmem_limit_bytes=8 * 2**20),
    )(scalars, carried, bias, own, other, *[p[0] for p in pieces])


def place_kernel(scalars, text, image, *refs):
    out, held, padded = refs[-3:]
    text_count, patch_count, width = text.shape[1], image.shape[0], image.shape[1]
    offset = scalars[OFFSET]
    shift = lax.rem(offset, 8)
    first = offset - shift
    chunk = tile_of(patch_count, 64, 8)
    sublane = lax.broadcasted_iota(jnp.int32, (1, 8, 128), 1)
    for start in range(0, width, 128):
        lanes = slice(start, start + 128)
        words = text[0, :, lanes].astype(F32)
        held[0:text_count, lanes] = words
        held[patch_count : patch_count + text_count, lanes] = words
        padded[8 : 8 + patch_count, lanes] = image[:, lanes].astype(F32)
        for row in range(0, patch_count + 8, chunk):
            size = min(chunk, patch_count + 8 - row)
            values = padded[row : row + size + 8, lanes].reshape(-1, 8, 128)
            turned = pltpu.roll(values, shift, 1)
            moved = jnp.where(sublane < shift, turned[:-1], turned[1:])
            window = pl.ds(pl.multiple_of(first + row, 8), size)
            if row == 0 or row + size > patch_count:
                place = lax.broadcasted_iota(jnp.int32, moved.shape, 0) * 8 + sublane + row
                kept = held[window, lanes].reshape(-1, 8, 128)
                moved = jnp.where((place >= shift) & (place < shift + patch_count), moved, kept)
            held[window, lanes] = moved.reshape(size, 128)
    out[0] = held[0 : text_count + patch_count].astype(out.dtype)


def place(scalars, text, image, sequence, mine):
    patch_count, half = image.shape
    text_count, width = text.shape[1], text.shape[2]
    length = text_count + patch_count
    tile = tile_of(half, 512, 128)
    steps = half // tile

    def side(i, s):
        return (s[CORE] if mine else 1 - s[CORE]) * steps + i

    operands = [text, image] + ([] if sequence is None else [sequence])
    return pl.pallas_call(
        place_kernel,
        grid_spec=pltpu.PrefetchScalarGridSpec(
            num_scalar_prefetch=1,
            grid=(steps,),
            in_specs=[
                pl.BlockSpec((1, text_count, tile), lambda i, s: (0, 0, side(i, s))),
                pl.BlockSpec((patch_count, tile), lambda i, s: (0, i)),
            ]
            + ([] if sequence is None else [pl.BlockSpec(memory_space=pl.ANY)]),
            out_specs=pl.BlockSpec((1, length, tile), lambda i, s: (0, 0, side(i, s))),
            scratch_shapes=[pltpu.VMEM((length + 8, tile), F32), pltpu.VMEM((patch_count + 16, tile), F32)],
        ),
        out_shape=jax.ShapeDtypeStruct((1, length, width), BF16),
        input_output_aliases={} if sequence is None else {3: 0},
        cost_estimate=pl.CostEstimate(flops=10**9, bytes_accessed=4 * length * half, transcendentals=0),
        compiler_params=pltpu.CompilerParams(vmem_limit_bytes=8 * 2**20),
    )(scalars, *operands)


def edge_pairs(rows, distance, parity):
    pairs = []
    for i in range(parity, rows - 1, 2):
        if i >= distance - 1:
            pairs.append((i, i + 1))
        if i + 1 <= rows - distance:
            pairs.append((i + 1, i))
    return pairs


def full_pairs(rows, cols, distance, parity):
    if distance == rows - 1:
        return [(i * cols + c, j * cols + c) for i, j in edge_pairs(rows, distance, parity) for c in range(cols)]
    busy = {min(pair) for pair in edge_pairs(rows, distance, parity)}
    pairs = []
    for row in range(rows):
        other = row + 1 if row in busy else row - 1 if row - 1 in busy else None
        for col in range(cols):
            target = row * cols + (col ^ 1) if other is None else other * cols + col
            pairs.append((row * cols + col, target))
    return pairs if busy else []


def arrivals(rows, row):
    order = []
    for distance in range(1, rows):
        for parity in (0, 1):
            for source, target in edge_pairs(rows, distance, parity):
                if target == row:
                    order.append((parity, distance, row - distance if source < target else row + distance))
    return order


def last_paths(rows):
    moves = {}
    for row in range(rows):
        parity, distance, origin = arrivals(rows, row)[-1]
        step = 1 if origin > row else -1
        for hop in range(distance):
            key = ((parity + hop) % 2, distance - hop)
            moves.setdefault(key, set()).add((row + (hop + 1) * step, row + hop * step))
    return moves


def arrange_kernel(piece_rows, scalars, *refs):
    parts, out, sems = refs[:-2], refs[-2], refs[-1]
    chip, core = scalars[PIECE] // piece_rows, scalars[CORE]
    copies = []
    for number, part in enumerate(parts):
        step, side = divmod(number, CORES)
        target = out.at[:, chip if step == 0 else 1 - chip, core if side == 0 else 1 - core]
        copies.append(pltpu.make_async_copy(part, target, sems.at[number]))
        copies[-1].start()
    for copy in copies:
        copy.wait()


def arrange(scalars, parts, piece_rows):
    images, patches, width = parts[0].shape
    shape = (images, len(parts) // CORES, CORES, patches, width)
    return pl.pallas_call(
        functools.partial(arrange_kernel, piece_rows),
        grid_spec=pltpu.PrefetchScalarGridSpec(
            num_scalar_prefetch=1,
            grid=(),
            in_specs=[pl.BlockSpec(memory_space=pl.ANY)] * len(parts),
            out_specs=pl.BlockSpec(shape, lambda s: (0,) * len(shape)),
            scratch_shapes=[pltpu.SemaphoreType.DMA((len(parts),))],
        ),
        out_shape=jax.ShapeDtypeStruct(shape, parts[0].dtype),
        cost_estimate=pl.CostEstimate(flops=10**9, bytes_accessed=4 * 2**20, transcendentals=0),
        compiler_params=pltpu.CompilerParams(vmem_limit_bytes=8 * 2**20),
    )(scalars, *parts)


def at_row(row, values):
    result = values[-1]
    for index in range(len(values) - 2, -1, -1):
        result = jnp.where(row == index, values[index], result)
    return result


def choose_kernel(first, which, *refs):
    choices, out, sem = refs[:-2], refs[-2], refs[-1]
    window = pl.ds(first, out.shape[0])
    for index, choice in enumerate(choices):

        @pl.when(which[0] == index)
        def _():
            pltpu.make_async_copy(choice.at[window], out, sem).start()

    pltpu.make_async_copy(choices[0].at[window], out, sem).wait()


def by_row(row, choices, first=0, count=None):
    count = count or choices[0].shape[0]
    distinct = []
    for choice in choices:
        if not any(choice is d for d in distinct):
            distinct.append(choice)
    if len(distinct) == 1:
        return distinct[0][first : first + count]
    which = at_row(row, [next(i for i, d in enumerate(distinct) if d is choice) for choice in choices])
    shape = (count, distinct[0].shape[1])
    return pl.pallas_call(
        functools.partial(choose_kernel, first),
        grid_spec=pltpu.PrefetchScalarGridSpec(
            num_scalar_prefetch=1,
            grid=(),
            in_specs=[pl.BlockSpec(memory_space=pl.ANY)] * len(distinct),
            out_specs=pl.BlockSpec(shape, lambda s: (0, 0)),
            scratch_shapes=[pltpu.SemaphoreType.DMA],
        ),
        out_shape=jax.ShapeDtypeStruct(shape, distinct[0].dtype),
        cost_estimate=pl.CostEstimate(flops=10**9, bytes_accessed=8 * shape[0] * shape[1], transcendentals=0),
        compiler_params=pltpu.CompilerParams(vmem_limit_bytes=8 * 2**20),
    )(which.astype(jnp.int32).reshape(1), *distinct)


def on_device(features, w_in, b_in, w_out, b_out, text, offsets):
    depths, rows, cols = lax.axis_size("depth"), lax.axis_size("row"), lax.axis_size("col")
    chips = cols // CORES
    row, col = lax.axis_index("row"), lax.axis_index("col")
    chip, core = col // CORES, col % CORES
    _, patch_count, part_width = features.shape
    block, out_width = w_out.shape
    half_block, half_out = block // CORES, out_width // CORES
    piece_rows = block // chips
    height = piece_rows // PIECES

    def to_core(value):
        return lax.ppermute(value, "col", [(i, i ^ 1) for i in range(cols)])

    def to_chip(value, step):
        return lax.ppermute(value, "col", [(i, (i + step * CORES) % cols) for i in range(cols)])

    def to_depth(value, step):
        return lax.ppermute(value, "depth", [(i, (i + step) % depths) for i in range(depths)])

    tables = [arrivals(rows, i) for i in range(rows)]
    blocks = [row] + [at_row(row, [t[k][2] for t in tables]) for k in range(rows - 1)]

    pieces = [
        lax.dynamic_slice(w_out, (chip * piece_rows + j * height, core * half_out), (height, half_out))
        for j in range(PIECES)
    ]
    moved = {(parity, 0, j): pieces[j] for parity in (0, 1) for j in range(PIECES)}
    for distance in range(1, rows):
        for j in range(PIECES):
            for parity in (0, 1):
                pairs = full_pairs(rows, cols, distance, parity)
                if pairs:
                    held = moved[1 - parity, distance - 1, j]
                    moved[parity, distance, j] = lax.ppermute(held, ("row", "col"), pairs)
    split = chips == CORES and height % 256 == 0
    if split:
        end = height // 2
        later = lax.optimization_barrier((w_out, pieces[0]))[0]
        spot = ((1 - chip) * piece_rows + piece_rows - end, core * half_out)
        extra = lax.dynamic_slice(later, spot, (end, half_out))
        carried = {}
        paths = last_paths(rows)
        for parity, distance in sorted(paths, key=lambda move: move[1]):
            if distance == 1:
                held = extra
                pairs = [(i * cols + c, j * cols + c) for i, j in sorted(paths[parity, 1]) for c in range(cols)]
            else:
                held = carried[1 - parity, distance - 1]
                pairs = full_pairs(rows, cols, distance, parity)
            carried[parity, distance] = lax.ppermute(held, ("row", "col"), pairs)
    stage_pieces = [None]
    starts = [chip * piece_rows] + [(chip - step) % chips * piece_rows for step in range(1, chips)]
    scalars = jnp.stack([core, offsets[0], *starts, *[b * CORES + core for b in blocks]])
    scalars = scalars.astype(jnp.int32)
    for k in range(1, rows):
        own, received = [], []
        for j in range(PIECES):
            choices = [moved[t[k - 1][:2] + (j,)] for t in tables]
            cut_short = split and k == rows - 1 and j == PIECES - 1
            count = height - end if cut_short else height
            chosen = by_row(row, choices, 0, count)
            own.append((chosen, PIECE, j * height))
            for step in range(1, chips):
                received.append((to_chip(chosen, step), PIECE + step, j * height))
            if cut_short:
                start = j * height + count
                own.append((by_row(row, choices, count, end), PIECE, start))
                chosen = by_row(row, [carried[t[k - 1][:2]] for t in tables])
                received.insert(0, (chosen, PIECE + 1, start))
        stage_pieces.append(own + received)

    by_chip = features.reshape(chips, CORES, patch_count, part_width)
    sent = [
        lax.dynamic_index_in_dim(by_chip, (chip + step) % chips, 0, keepdims=False) for step in range(chips)
    ]
    tokens = []
    for away in range(depths):
        got = []
        for step in range(chips):
            pairs = [
                (d * cols + i, (d + away) % depths * cols + (i + step * CORES) % cols)
                for d in range(depths)
                for i in range(cols)
            ]
            got.append(lax.ppermute(sent[step], ("depth", "col"), pairs) if away or step else sent[0])
        with_other = [(value, to_core(value)) for value in got]
        if chips == 2:
            part = arrange(scalars, [value for pair in with_other for value in pair], piece_rows)
        else:
            part = jnp.zeros((CORES, chips, CORES, patch_count, part_width), features.dtype)
            for step, pair in enumerate(with_other):
                pair = jnp.where(core == 0, jnp.stack(pair, 1), jnp.stack(pair[::-1], 1))[:, None]
                part = lax.dynamic_update_slice(part, pair, (0, (chip - step) % chips, 0, 0, 0))
        tokens.append(part.reshape(-1, part_width))

    bias_in = b_in.reshape(rows * CORES, 1, half_block)
    hidden = []
    columns = [b * block + core * half_block for b in blocks]
    cuts = [lax.dynamic_slice_in_dim(w_in, columns[0], half_block, 1)]
    later = lax.optimization_barrier((w_in, cuts[0]))[0]
    cuts += [lax.dynamic_slice_in_dim(later, column, half_block, 1) for column in columns[1:]]
    for k in range(rows):
        own = cuts[k]
        weights = [own] + [to_depth(own, step) for step in range(1, depths)]
        value = hidden_part(scalars, tokens, weights, bias_in, PIECE + chips + k)
        hidden.append((value, to_core(value)))

    bias_out = lax.dynamic_slice_in_dim(b_out, core * half_out, half_out).reshape(1, half_out)
    for k in range(rows - split):
        stage = (*hidden[k], w_out if k == 0 else None, stage_pieces[k] or [])
        total = product(scalars, [stage], total if k else None)
    if split:
        last = stage_pieces[-1]
        total = third(scalars, total, *hidden[-1], last[:-1])
        sent = finish(scalars, 0, total, bias_out, *hidden[-1], last[-1:])
        kept = finish(scalars, 1, total, bias_out, *hidden[-1], last[-1:])
    else:
        result = (total + bias_out).astype(BF16).reshape(CORES, -1, half_out)
        sent = lax.dynamic_index_in_dim(result, 1 - core, 0, keepdims=False)
        kept = lax.dynamic_index_in_dim(result, core, 0, keepdims=False)
    arrived = to_core(sent)
    sequence = place(scalars, text, kept, None, True)
    return place(scalars, text, arrived, sequence, False)


def solution(mesh):
    return jax.shard_map(
        on_device,
        mesh=mesh,
        in_specs=(
            P("row", "col", "depth"),
            P("depth", None),
            P(),
            P("row", "depth"),
            P("depth"),
            P(("row", "col"), None, "depth"),
            P(("row", "col")),
        ),
        out_specs=P(("row", "col"), None, "depth"),
        check_vma=False,
    )
```
